8 devices in a mesh: dp: 1 (over z), sp: 8 (over y, x, core).
Axes of the slice: x: 2, y: 2, z: 1, core: 2. Of those that a mesh axis runs over, the one named last changes fastest.
Arguments:
- x_text: bfloat16 [12288, 4096], P(('dp', 'sp'))
- patches: bfloat16 [16, 576, 588], P(('dp', 'sp'))
- img_start: int32 [16], P('dp')
- w_patch: bfloat16 [588, 1024], replicated
- pos_table: bfloat16 [576, 1024], replicated
- vit_ln1: bfloat16 [1024], replicated
- w_vqkv: bfloat16 [1024, 3, 16, 64], replicated
- w_vout: bfloat16 [16, 64, 1024], replicated
- vit_ln2: bfloat16 [1024], replicated
- w_vfc1: bfloat16 [1024, 4096], replicated
- w_vfc2: bfloat16 [4096, 1024], replicated
- w_proj1: bfloat16 [1024, 4096], replicated
- w_proj2: bfloat16 [4096, 4096], replicated
- rms_attn: bfloat16 [4096], replicated
- w_query: bfloat16 [4096, 32, 128], replicated
- w_key: bfloat16 [4096, 32, 128], replicated
- w_value: bfloat16 [4096, 32, 128], replicated
- w_out: bfloat16 [32, 128, 4096], replicated
- rms_mlp: bfloat16 [4096], replicated
- w_gate: bfloat16 [4096, 11008], replicated
- w_up: bfloat16 [4096, 11008], replicated
- w_down: bfloat16 [11008, 4096], replicated
Outputs:
- output: bfloat16 [12288, 4096], P(('dp', 'sp'))
All inputs are finite; a program needn't handle non-finite values.
Results may differ from the reference program's by a relative error of at most 0.013174.
Values are sent between devices in bfloat16 or wider.
A program may use at most 2 GiB of HBM per device.

```python
import jax
import jax.numpy as jnp
from jax import lax

D = 4096
HEADS = 32
KV_HEADS = 32
HEAD = 128
FF = 11008
DV = 1024
VHEADS = 16
PATCH = 576
CH = 588
SEQ_DEV = 1536
IMG_DEV = 2
GROUP = 8

SEQ_LEN = SEQ_DEV * GROUP
N_IMG = IMG_DEV * GROUP
BLOCK_LEN = SEQ_DEV // 2
SEG_LEN = SEQ_DEV // IMG_DEV
VHEAD = DV // VHEADS
Q_PER_KV = HEADS // KV_HEADS
ROPE_BASE = 10000.0
RMS_EPS = 1e-6
LN_EPS = 1e-5


def draw_weight(key, shape, fan_in):
    return (jax.random.normal(key, shape, jnp.float32) * fan_in ** -0.5).astype(jnp.bfloat16)


def draw_gain(key, width):
    return (1.0 + 0.3 * jax.random.normal(key, (width,), jnp.float32)).astype(jnp.bfloat16)


def draw_starts(key):
    key_shift, key_seg, key_off = jax.random.split(key, 3)
    shift_perm = jax.random.permutation(key_shift, GROUP)
    shifts = shift_perm[jnp.arange(IMG_DEV) % GROUP]
    seg_perm = jax.random.permutation(key_seg, IMG_DEV)
    offsets = jax.random.randint(key_off, (GROUP, IMG_DEV), 0, SEG_LEN - PATCH + 1)
    dest_dev = (jnp.arange(GROUP)[:, None] + shifts[None, :]) % GROUP
    local_row = seg_perm[None, :] * SEG_LEN + offsets
    block_id = jnp.where(local_row < BLOCK_LEN, dest_dev, 2 * GROUP - 1 - dest_dev)
    starts = block_id * BLOCK_LEN + local_row % BLOCK_LEN
    return starts.reshape(N_IMG).astype(jnp.int32)


def setup_inputs(seed: int = 0, part: int = 0) -> dict:
    part_keys = jax.random.split(jax.random.fold_in(jax.random.key(seed), part), 4)
    shared = jax.random.split(jax.random.key(seed + 1), 19)
    noise = jax.random.normal(part_keys[0], (2 * GROUP, BLOCK_LEN, D), jnp.float32)
    offsets = jax.random.normal(part_keys[1], (2 * GROUP, 1, D), jnp.float32)
    x_text = (noise + offsets).reshape(SEQ_LEN, D).astype(jnp.bfloat16)
    patches = jax.random.normal(part_keys[2], (N_IMG, PATCH, CH), jnp.float32).astype(jnp.bfloat16)
    return {
        'x_text': x_text,
        'patches': patches,
        'img_start': draw_starts(part_keys[3]),
        'w_patch': draw_weight(shared[0], (CH, DV), CH),
        'pos_table': jax.random.normal(shared[1], (PATCH, DV), jnp.float32).astype(jnp.bfloat16),
        'vit_ln1': draw_gain(shared[2], DV),
        'w_vqkv': draw_weight(shared[3], (DV, 3, VHEADS, VHEAD), DV),
        'w_vout': draw_weight(shared[4], (VHEADS, VHEAD, DV), DV),
        'vit_ln2': draw_gain(shared[5], DV),
        'w_vfc1': draw_weight(shared[6], (DV, 4 * DV), DV),
        'w_vfc2': draw_weight(shared[7], (4 * DV, DV), 4 * DV),
        'w_proj1': draw_weight(shared[8], (DV, D), DV),
        'w_proj2': draw_weight(shared[9], (D, D), D),
        'rms_attn': draw_gain(shared[10], D),
        'w_query': draw_weight(shared[11], (D, HEADS, HEAD), D),
        'w_key': draw_weight(shared[12], (D, KV_HEADS, HEAD), D),
        'w_value': draw_weight(shared[13], (D, KV_HEADS, HEAD), D),
        'w_out': draw_weight(shared[14], (HEADS, HEAD, D), HEADS * HEAD),
        'rms_mlp': draw_gain(shared[15], D),
        'w_gate': draw_weight(shared[16], (D, FF), D),
        'w_up': draw_weight(shared[17], (D, FF), D),
        'w_down': draw_weight(shared[18], (FF, D), FF),
    }


def layer_norm(values, gain):
    wide = values.astype(jnp.float32)
    row_mean = wide.mean(-1, keepdims=True)
    centered = wide - row_mean
    row_var = (centered * centered).mean(-1, keepdims=True)
    return (centered * lax.rsqrt(row_var + LN_EPS) * gain.astype(jnp.float32)).astype(jnp.bfloat16)


def rms_norm(values, gain):
    wide = values.astype(jnp.float32)
    mean_sq = (wide * wide).mean(-1, keepdims=True)
    return (wide * lax.rsqrt(mean_sq + RMS_EPS) * gain.astype(jnp.float32)).astype(jnp.bfloat16)


def apply_rope(values, positions):
    half_dim = values.shape[-1] // 2
    inv_freq = ROPE_BASE ** (-jnp.arange(half_dim).astype(jnp.float32) * 2.0 / values.shape[-1])
    angles = positions[:, None] * inv_freq[None, :]
    cosine = jnp.cos(angles)[:, None, :]
    sine = jnp.sin(angles)[:, None, :]
    first = values[..., :half_dim].astype(jnp.float32)
    second = values[..., half_dim:].astype(jnp.float32)
    return jnp.concatenate([first * cosine - second * sine, second * cosine + first * sine], axis=-1).astype(jnp.bfloat16)


def encode_image(pixels, w_patch, pos_table, vit_ln1, w_vqkv, w_vout, vit_ln2, w_vfc1, w_vfc2, w_proj1, w_proj2):
    embedded = (jnp.dot(pixels, w_patch, preferred_element_type=jnp.float32) + pos_table.astype(jnp.float32)).astype(jnp.bfloat16)
    normed = layer_norm(embedded, vit_ln1)
    qkv_all = jnp.einsum('pv,vthd->tphd', normed.astype(jnp.float32), w_vqkv.astype(jnp.float32)).astype(jnp.bfloat16)
    scores = jnp.einsum('qhd,khd->hqk', qkv_all[0].astype(jnp.float32), qkv_all[1].astype(jnp.float32)) * VHEAD ** -0.5
    attn_prob = jax.nn.softmax(scores, axis=-1).astype(jnp.bfloat16)
    context = jnp.einsum('hqk,khd->qhd', attn_prob.astype(jnp.float32), qkv_all[2].astype(jnp.float32)).astype(jnp.bfloat16)
    hidden = (embedded.astype(jnp.float32) + jnp.einsum('qhd,hdv->qv', context.astype(jnp.float32), w_vout.astype(jnp.float32))).astype(jnp.bfloat16)
    normed_mlp = layer_norm(hidden, vit_ln2)
    hidden_act = jax.nn.gelu(jnp.dot(normed_mlp, w_vfc1, preferred_element_type=jnp.float32)).astype(jnp.bfloat16)
    vision = (hidden.astype(jnp.float32) + jnp.dot(hidden_act, w_vfc2, preferred_element_type=jnp.float32)).astype(jnp.bfloat16)
    proj_mid = jax.nn.gelu(jnp.dot(vision, w_proj1, preferred_element_type=jnp.float32)).astype(jnp.bfloat16)
    return jnp.dot(proj_mid, w_proj2, preferred_element_type=jnp.float32).astype(jnp.bfloat16)


def to_natural(stored_rows):
    blocks = stored_rows.reshape(GROUP, 2, BLOCK_LEN, D)
    return jnp.concatenate([blocks[:, 0], blocks[::-1, 1]], axis=0).reshape(SEQ_LEN, D)


def to_stored(natural_rows):
    blocks = natural_rows.reshape(2 * GROUP, BLOCK_LEN, D)
    return jnp.stack([blocks[:GROUP], blocks[GROUP:][::-1]], axis=1).reshape(SEQ_LEN, D)


def decoder_layer(hidden, rms_attn, w_query, w_key, w_value, w_out, rms_mlp, w_gate, w_up, w_down):
    positions = jnp.arange(SEQ_LEN).astype(jnp.float32)
    normed = rms_norm(hidden, rms_attn).astype(jnp.float32)
    queries = apply_rope(jnp.einsum('sd,dhe->she', normed, w_query.astype(jnp.float32)).astype(jnp.bfloat16), positions)
    key_rows = apply_rope(jnp.einsum('sd,dhe->she', normed, w_key.astype(jnp.float32)).astype(jnp.bfloat16), positions)
    value_rows = jnp.einsum('sd,dhe->she', normed, w_value.astype(jnp.float32)).astype(jnp.bfloat16)
    q_blocks = queries.reshape(2 * GROUP, BLOCK_LEN, KV_HEADS, Q_PER_KV, HEAD)
    k_blocks = key_rows.reshape(2 * GROUP, BLOCK_LEN, KV_HEADS, HEAD)
    v_blocks = value_rows.reshape(2 * GROUP, BLOCK_LEN, KV_HEADS, HEAD)
    w_out_grouped = w_out.reshape(KV_HEADS, Q_PER_KV, HEAD, D).astype(jnp.float32)

    def attend_query_block(inputs):
        block_idx, q_block = inputs
        q_pos = block_idx * BLOCK_LEN + jnp.arange(BLOCK_LEN)
        q_wide = q_block.astype(jnp.float32)

        def body(online_state, kv_inputs):
            run_max, run_sum, run_acc = online_state
            key_idx, k_block, v_block = kv_inputs
            k_pos = key_idx * BLOCK_LEN + jnp.arange(BLOCK_LEN)
            scores = jnp.einsum('qhgd,khd->hgqk', q_wide, k_block.astype(jnp.float32)) * HEAD ** -0.5
            allowed = k_pos[None, :] <= q_pos[:, None]
            scores = jnp.where(allowed, scores, -1e30)
            new_max = jnp.maximum(run_max, scores.max(axis=-1))
            exp_scores = jnp.where(allowed, jnp.exp(scores - new_max[..., None]), 0.0)
            factor = jnp.exp(run_max - new_max)
            new_sum = run_sum * factor + exp_scores.sum(axis=-1)
            new_acc = run_acc * factor[..., None] + jnp.einsum('hgqk,khd->hgqd', exp_scores.astype(jnp.bfloat16).astype(jnp.float32), v_block.astype(jnp.float32))
            return (new_max, new_sum, new_acc), None

        init_state = (jnp.full((KV_HEADS, Q_PER_KV, BLOCK_LEN), -jnp.inf, jnp.float32), jnp.zeros((KV_HEADS, Q_PER_KV, BLOCK_LEN), jnp.float32), jnp.zeros((KV_HEADS, Q_PER_KV, BLOCK_LEN, HEAD), jnp.float32))
        final, unused = lax.scan(body, init_state, (jnp.arange(2 * GROUP), k_blocks, v_blocks))
        context = (final[2] / final[1][..., None]).astype(jnp.bfloat16)
        return jnp.einsum('hgqd,hgde->qe', context.astype(jnp.float32), w_out_grouped)

    attn_out = lax.map(attend_query_block, (jnp.arange(2 * GROUP), q_blocks)).reshape(SEQ_LEN, D)
    mid_rows = (hidden.astype(jnp.float32) + attn_out).astype(jnp.bfloat16)
    normed_mlp = rms_norm(mid_rows, rms_mlp)
    gate_act = jnp.dot(normed_mlp, w_gate, preferred_element_type=jnp.float32)
    up_proj = jnp.dot(normed_mlp, w_up, preferred_element_type=jnp.float32)
    mixed = (jax.nn.silu(gate_act) * up_proj).astype(jnp.bfloat16)
    return (mid_rows.astype(jnp.float32) + jnp.dot(mixed, w_down, preferred_element_type=jnp.float32)).astype(jnp.bfloat16)


def reference(x_text, patches, img_start, w_patch, pos_table, vit_ln1, w_vqkv, w_vout, vit_ln2, w_vfc1, w_vfc2, w_proj1, w_proj2, rms_attn, w_query, w_key, w_value, w_out, rms_mlp, w_gate, w_up, w_down):
    def encode_one(pixels):
        return encode_image(pixels, w_patch, pos_table, vit_ln1, w_vqkv, w_vout, vit_ln2, w_vfc1, w_vfc2, w_proj1, w_proj2)

    img_rows = lax.map(encode_one, patches)
    natural = to_natural(x_text)
    seq_rows = (img_start[:, None] + jnp.arange(PATCH)[None, :]).reshape(-1)
    hidden = natural.at[seq_rows].set(img_rows.reshape(N_IMG * PATCH, D))
    result = decoder_layer(hidden, rms_attn, w_query, w_key, w_value, w_out, rms_mlp, w_gate, w_up, w_down)
    return to_stored(result)
```

```python
import functools

import jax
import jax.numpy as jnp
from jax import lax
from jax.experimental import pallas as pl
from jax.experimental.pallas import tpu as pltpu
from jax.sharding import PartitionSpec as P

ROPE_BASE = 10000.0
RMS_EPS = 1e-6
LN_EPS = 1e-5
C = (128 ** -0.5) * 1.4426950408889634
TQ, TK = 1024, 512
NEG = -1e30
BL = 768
HALF = 8 * BL
f32 = jnp.float32
bf16 = jnp.bfloat16


def layer_norm(values, gain):
    wide = values.astype(f32)
    centered = wide - wide.mean(-1, keepdims=True)
    row_var = (centered * centered).mean(-1, keepdims=True)
    return (centered * lax.rsqrt(row_var + LN_EPS) * gain.astype(f32)).astype(bf16)


def rms_norm(values, gain):
    wide = values.astype(f32)
    mean_sq = (wide * wide).mean(-1, keepdims=True)
    return (wide * lax.rsqrt(mean_sq + RMS_EPS) * gain.astype(f32)).astype(bf16)


def dot(a, b):
    return jnp.dot(a, b, preferred_element_type=f32)


def encode_image(pixels, w_patch, pos_table, ln1, w_vqkv, w_vout, ln2, w_fc1, w_fc2, w_proj1, w_proj2):
    embedded = (dot(pixels, w_patch) + pos_table.astype(f32)).astype(bf16)
    normed = layer_norm(embedded, ln1)
    qkv = jnp.einsum('pv,vthd->thpd', normed, w_vqkv, preferred_element_type=f32).astype(bf16)
    scores = jnp.einsum('hqd,hkd->hqk', qkv[0], qkv[1], preferred_element_type=f32) * w_vqkv.shape[3] ** -0.5
    prob = jax.nn.softmax(scores, axis=-1).astype(bf16)
    context = jnp.einsum('hqk,hkd->hqd', prob, qkv[2], preferred_element_type=f32).astype(bf16)
    hidden = (embedded.astype(f32) + jnp.einsum('hqd,hdv->qv', context, w_vout, preferred_element_type=f32)).astype(bf16)
    act = jax.nn.gelu(dot(layer_norm(hidden, ln2), w_fc1)).astype(bf16)
    vision = (hidden.astype(f32) + dot(act, w_fc2)).astype(bf16)
    mid = jax.nn.gelu(dot(vision, w_proj1)).astype(bf16)
    return dot(mid, w_proj2).astype(bf16)


def rope_tables():
    half = 64
    inv_freq = ROPE_BASE ** (-jnp.arange(half).astype(f32) * 2.0 / 128)
    ang = jnp.arange(2 * HALF).astype(f32)[:, None] * inv_freq[None]
    c, s = jnp.cos(ang), jnp.sin(ang)
    return jnp.concatenate([c, c], 1), jnp.concatenate([-s, s], 1)


def _colmax(s): return jnp.max(s,axis=0,keepdims=True)
def _colsum8(p): return jnp.sum(p.reshape(p.shape[0]//8,8,p.shape[1]),axis=0)

def attn_kernel(mode, *refs):
    causal = mode != 'B1'
    if mode=='A':
        q_ref,k_ref,v_ref,cq,sq,o_ref,qT,ks,vT,s0,s1,acc=refs; ck,sk=cq,sq
    elif mode=='B1':
        q_ref,k_ref,v_ref,cq,sq,ck,sk,oa_ref,oml_ref,qT,ks,vT,s0,s1,acc=refs
    else:
        q_ref,k_ref,v_ref,cq,sq,ia_ref,iml_ref,o_ref,qT,ks,vT,s0,s1,acc=refs; ck,sk=cq,sq
    sb=(s0,s1)
    def A(x): return pl.multiple_of(x,TK)
    def rope(x,cos,sin):
        xf=x.astype(f32)
        return (xf*cos+pltpu.roll(xf,64,1)*sin).astype(bf16)
    def prep(b,_):
        kb = 7-b if mode=='B2' else b
        qb = b if mode=='A' else 7-b
        r=pl.multiple_of(kb*BL,BL)
        ks[pl.ds(r,BL),:]=rope(k_ref[b,0],ck[pl.ds(r,BL),:],sk[pl.ds(r,BL),:])
        vT[:,pl.ds(r,BL)]=v_ref[b,0].T
        rq=pl.multiple_of(qb*BL,BL)
        qr=rope(q_ref[b,0],cq[pl.ds(rq,BL),:],sq[pl.ds(rq,BL),:]).astype(f32)*C
        hi=qr.astype(bf16); lo=(qr-hi.astype(f32)).astype(bf16)
        qT[0:128,pl.ds(rq,BL)]=hi.T
        qT[128:256,pl.ds(rq,BL)]=lo.T
        return 0
    lax.fori_loop(0,8,prep,0)

    def S1(j,buf,c0,w=TQ,o=0,mx=True):
        k=ks[pl.ds(j,TK),:]
        s=jnp.dot(jnp.concatenate([k,k],axis=1),qT[:,pl.ds(c0,w)],preferred_element_type=f32)
        buf[:,o:o+w]=s
        return _colmax(s) if mx else None
    def S23(j,buf,m,l,mt,mask=None,o=0,w=TQ):
        s=buf[:,o:o+w]
        if mask is not None:
            s=jnp.where(mask,s,NEG)
            mt=_colmax(s)
        mn=mt if m is None else jnp.maximum(m,mt)
        p=jnp.exp2(s-mn)
        ps=_colsum8(p)
        pv=jnp.dot(vT[:,pl.ds(j,TK)],p.astype(bf16),preferred_element_type=f32)
        if m is None:
            acc[:,o:o+w]=pv
            return mn,ps
        al=jnp.exp2(m-mn)
        acc[:,o:o+w]=acc[:,o:o+w]*al+pv
        return mn,l*al+ps
    H2=TQ-TK
    def finish(i,l):
        ls=jnp.sum(l,axis=0,keepdims=True)
        o=(acc[...]*(1.0/ls)).astype(bf16)
        for u in range(TQ//256):
            pc=i*(TQ//256)+u
            blk=pc//3; off=pl.multiple_of((pc%3)*256,256)
            if mode=='B2': blk=7-blk
            o_ref[blk,pl.ds(off,256),:]=o[:,u*256:(u+1)*256].T
    def tail(c0,d0,m,l):
        rows=lax.broadcasted_iota(jnp.int32,(TK,TQ),0); cols=lax.broadcasted_iota(jnp.int32,(TK,TQ),1)
        mk=rows<=cols
        S1(A(d0+TK),sb[1],A(c0+TK),w=H2,o=TK,mx=False)
        m,l=S23(d0,sb[0],m,l,None,mask=mk)
        m2,l2=S23(A(d0+TK),sb[1],m[:,TK:],l[:,TK:],None,mask=mk[:,:H2],o=TK,w=H2)
        return jnp.concatenate([l[:,:TK],l2],axis=1)
    def init(c0):
        if mode=='B2':
            acc[...]=ia_ref[0,:,pl.ds(c0,TQ)]
            return iml_ref[0,8:9,pl.ds(c0,TQ)],iml_ref[0,0:8,pl.ds(c0,TQ)]
        acc[...]=jnp.zeros((128,TQ),f32)
        return jnp.full((1,TQ),NEG,f32),jnp.zeros((8,TQ),f32)
    def pair(j,c,c0,last=False):
        m,l,mt=c
        mtn=S1(A(j+TK),sb[1],c0)
        m,l=S23(A(j),sb[0],m,l,mt)
        mt2=None if last else S1(A(j+2*TK),sb[0],c0)
        m,l=S23(A(j+TK),sb[1],m,l,mtn)
        return m,l,mt2
    def qtile(i,_):
        c0=pl.multiple_of(i*TQ,TQ)
        m,l=init(c0)
        mt0=S1(0,sb[0],c0)
        def body(t,c):
            j=4*t*TK
            return pair(j+2*TK,pair(j,c,c0),c0)
        if causal:
            n=2*i
            n4=n//4
            c=lax.fori_loop(0,n4,body,(m,l,mt0))
            m,l,mt=lax.fori_loop(2*n4,n//2,lambda t,c: pair(2*t*TK,c,c0),c)
            l=tail(c0,A(i*TQ),m,l)
            finish(i,l)
        else:
            n=HALF//TK
            c=lax.fori_loop(0,n//4-1,body,(m,l,mt0))
            c=pair((n-4)*TK,c,c0)
            m,l,_u=pair((n-2)*TK,c,c0,last=True)
            oa_ref[0,:,pl.ds(c0,TQ)]=acc[...]
            oml_ref[0,0:8,pl.ds(c0,TQ)]=l
            oml_ref[0,8:16,pl.ds(c0,TQ)]=jnp.broadcast_to(m,(8,TQ))
        return 0
    nq=HALF//TQ
    if causal:
        if mode=='B2': m,l=init(0)
        else: m,l=None,None
        S1(0,sb[0],0,mx=False)
        l=tail(0,0,m,l)
        finish(0,l)
        lax.fori_loop(1,nq,qtile,0)
    else:
        lax.fori_loop(0,nq,qtile,0)

def attn_call(mode,q,k,v,tabs,state=None):
    H=q.shape[1]
    bs=pl.BlockSpec((8,1,BL,128),lambda h:(0,h,0,0))
    ts=pl.BlockSpec((HALF,128),lambda h:(0,0),pipeline_mode=pl.Buffered(1))
    sa=pl.BlockSpec((1,128,HALF),lambda h:(h,0,0)); sml=pl.BlockSpec((1,16,HALF),lambda h:(h,0,0))
    ins=[q,k,v,*tabs]; in_specs=[bs]*3+[ts]*len(tabs)
    units=HALF*HALF*H*(1 if mode=='B1' else 0.55)
    by=3*q.size*2+8*BL*128*2*H
    if mode=='B2':
        ins+=list(state); in_specs+=[sa,sml]
    if mode=='B1':
        out_shape=(jax.ShapeDtypeStruct((H,128,HALF),f32),jax.ShapeDtypeStruct((H,16,HALF),f32)); out_specs=(sa,sml)
    else:
        out_shape=jax.ShapeDtypeStruct((8,BL,H*128),bf16); out_specs=pl.BlockSpec((8,BL,128),lambda h:(0,0,h))
    return pl.pallas_call(functools.partial(attn_kernel,mode),grid=(H,),in_specs=in_specs,out_specs=out_specs,out_shape=out_shape,
        scratch_shapes=[pltpu.VMEM((256,HALF),bf16),pltpu.VMEM((HALF,128),bf16),pltpu.VMEM((128,HALF),bf16),
            pltpu.VMEM((TK,TQ),f32),pltpu.VMEM((TK,TQ),f32),pltpu.VMEM((128,TQ),f32)],
        compiler_params=pltpu.CompilerParams(dimension_semantics=("arbitrary",),vmem_limit_bytes=56<<20),
        cost_estimate=pl.CostEstimate(flops=int(1100*units),bytes_accessed=by,transcendentals=int(units)),
        name="attn_"+mode)(*ins)


def after(x, *deps):
    return lax.optimization_barrier((x,) + deps)[0]


def route_patches(pixels, starts, me):
    blk = starts // BL
    everyone = lax.all_gather(pixels, 'sp', axis=0, tiled=True)
    order = jnp.arange(16)
    picks = []
    for mine in (me, 15 - me):
        hit = blk == mine
        picks.append(lax.dynamic_index_in_dim(everyone, jnp.sum(jnp.where(hit, order, 0)), keepdims=False))
        picks.append(jnp.sum(jnp.where(hit, starts % BL, 0)))
    return picks


def exchange(x):
    return lax.all_to_all(x, 'sp', 0, 0, tiled=True)


def solution(mesh):
    def local_program(x_rows, pixels, starts, w_patch, pos_table, vit_ln1, w_vqkv, w_vout, vit_ln2, w_fc1, w_fc2, w_proj1, w_proj2, rms_attn, w_query, w_key, w_value, w_out, rms_mlp, w_gate, w_up, w_down):
        me = lax.axis_index('sp')
        px_a, off_a, px_b, off_b = route_patches(pixels, starts, me)
        cos, sin = rope_tables()
        tab_a, tab_b = (cos[:HALF], sin[:HALF]), (cos[HALF:], sin[HALF:])
        enc = lambda px: encode_image(px, w_patch, pos_table, vit_ln1, w_vqkv, w_vout, vit_ln2, w_fc1, w_fc2, w_proj1, w_proj2)
        w_out2 = w_out.reshape(8, 512, 4096)

        def place(rows, img, off):
            h0 = lax.dynamic_update_slice(rows, img, (off, 0))
            return h0, rms_norm(h0, rms_attn)

        def project(n1, w):
            y = jnp.einsum('sd,dhe->hse', n1, w, preferred_element_type=f32).astype(bf16)
            return exchange(y.reshape(8, 4, BL, 128))

        def finish(ctx, h0):
            mid = (h0.astype(f32) + jnp.einsum('sqc,scd->qd', ctx, w_out2, preferred_element_type=f32)).astype(bf16)
            n2 = rms_norm(mid, rms_mlp)
            y = (jax.nn.silu(dot(n2, w_gate)) * dot(n2, w_up)).astype(bf16)
            return (mid.astype(f32) + dot(y, w_down)).astype(bf16)

        h0a, n1a = place(x_rows[:BL], enc(px_a), off_a)
        ka, va, qa = project(n1a, w_key), project(n1a, w_value), project(n1a, w_query)
        h0b, n1b = place(x_rows[BL:], enc(px_b), off_b)
        qb, kb, vb = project(n1b, w_query), project(n1b, w_key), project(n1b, w_value)
        ctx_a = exchange(attn_call('A', qa, ka, va, tab_a))
        state = attn_call('B1', qb, ka, va, tab_b + tab_a)
        ctx_b = exchange(attn_call('B2', qb, kb, vb, tab_b, state))
        out_a = finish(ctx_a, h0a)
        out_b = finish(ctx_b, h0b)
        return jnp.concatenate([out_a, out_b], axis=0)

    row_spec = P(('dp', 'sp'), None)
    in_specs = (row_spec, P(('dp', 'sp'), None, None), P('dp')) + (P(),) * 19
    return jax.shard_map(local_program, mesh=mesh, in_specs=in_specs, out_specs=row_spec, check_vma=False)
```
